32 devices in a mesh: level: 4 (over z), dev: 8 (over y, x, core).
Axes of the slice: x: 2, y: 2, z: 4, core: 2. Of those that a mesh axis runs over, the one named last changes fastest.
Arguments:
- fields: float32 [4, 128, 12, 128], P('level', 'dev'), may hold values from -6 to 6
- own_src: int32 [4, 128], P('level', 'dev'), may hold values from 0 to 15
- own_weight: bfloat16 [4, 128, 128, 128], P('level', 'dev'), may hold values from 0 to 1, as said below
- send_block: int32 [4, 8, 8, 2], P('level', 'dev'), may hold values from 0 to 15
- send_target: int32 [4, 8, 8, 2], P('level', 'dev'), may hold values from 0 to 15
- send_count: int32 [4, 8, 8], P('level', 'dev'), may hold values from 0 to 2, as said below
- send_weight: bfloat16 [4, 8, 8, 2, 128, 128], P('level', 'dev'), may hold values from 0 to 1, as said below
- left_block: int32 [4, 8, 4, 2], P('level', 'dev'), may hold values from 0 to 15
- left_target: int32 [4, 8, 4, 2], P('level', 'dev'), may hold values from 0 to 15
- left_count: int32 [4, 8, 4], P('level', 'dev'), may hold values from 0 to 2, as said below
- left_weight: bfloat16 [4, 8, 4, 2, 128, 128], P('level', 'dev'), may hold values from 0 to 1, as said below
Outputs:
- remapped: float32 [4, 128, 12, 128], P('level', 'dev')
- totals: float32 [12], replicated
The draws below stay inside these ranges and needn't reach their ends.
Inputs may be any that keep to these rules, and one draw needn't show every extreme that they name: send_count[l, s, s] = 0; for every level some receiver device gets 2 live slots from every other device of the level. left_count[m, q, m] = 0; for every device index some receiver level gets 2 live slots from every other level. `own_weight`: nonnegative; entry [k, i] is zero where old cell k and new cell i differ by more than 3; each column sums to a positive intersect fraction of at most 1. `send_weight`: nonnegative; entry [k, i] is zero where old cell k and new cell i differ by more than 3; each column sums to a positive intersect fraction of at most 1. `left_weight`: nonnegative; entry [k, i] is zero where old cell k and new cell i differ by more than 3; each column sums to a positive intersect fraction of at most 1.
All inputs are finite; a program needn't handle non-finite values.
Results may differ from the reference program's by a relative error of at most 0.0045.
Values may be sent and summed in bfloat16 or wider, within the bound.
A program may use at most 64 MiB of HBM per device.

```python
import jax
import jax.numpy as jnp
from jax import lax

COMP = 12
CELLS = 128
HALF = 3
BLK_DEV = 16
CAP = 2
LCAP = 2
PEERS = 8
LEVELS = 4
BLOCKS = 128


def band_fractions(key, lead):
    first, second, third = jax.random.split(key, 3)
    shape = lead + (CELLS, CELLS)
    rowpos = lax.broadcasted_iota(jnp.int32, shape, len(lead))
    colpos = lax.broadcasted_iota(jnp.int32, shape, len(lead) + 1)
    spread = jnp.abs(rowpos - colpos)
    middle = jax.random.uniform(first, shape, jnp.float32, 2.0, 3.0)
    beside = jax.random.uniform(second, shape, jnp.float32, 0.3, 1.0)
    raw = jnp.where(spread == 0, middle, jnp.where(spread <= HALF, beside, jnp.zeros_like(beside)))
    fraction = jax.random.uniform(third, lead + (1, CELLS), jnp.float32, 0.2, 0.8)
    return raw / jnp.sum(raw, axis=-2, keepdims=True) * fraction


def draw_own_weight(key, part):
    whole = band_fractions(jax.random.fold_in(key, 11), (LEVELS, BLOCKS))
    return whole.astype(jnp.bfloat16)


def draw_send_weight(key, part):
    whole = band_fractions(jax.random.fold_in(key, 23), (LEVELS, PEERS, PEERS, CAP))
    return whole.astype(jnp.bfloat16)


def draw_left_weight(key, part):
    whole = band_fractions(jax.random.fold_in(key, 37), (LEVELS, PEERS, LEVELS, LCAP))
    return whole.astype(jnp.bfloat16)


def draw_send_count(key, part):
    shape = (LEVELS, PEERS, PEERS)
    base = jax.random.randint(key, shape, 0, CAP + 1)
    lvl = lax.broadcasted_iota(jnp.int32, shape, 0)
    src = lax.broadcasted_iota(jnp.int32, shape, 1)
    dst = lax.broadcasted_iota(jnp.int32, shape, 2)
    heavy = (7 * lvl + 3) % PEERS
    near = ((dst - src) % PEERS == 1) | ((src - dst) % PEERS == 1)
    full = (dst == heavy) | near
    out = jnp.where(full, CAP, base)
    return jnp.where(src == dst, 0, out).astype(jnp.int32)


def draw_left_count(key, part):
    shape = (LEVELS, PEERS, LEVELS)
    base = jax.random.randint(key, shape, 0, LCAP + 1)
    src = lax.broadcasted_iota(jnp.int32, shape, 0)
    dev = lax.broadcasted_iota(jnp.int32, shape, 1)
    dst = lax.broadcasted_iota(jnp.int32, shape, 2)
    heavy = (5 * dev + 1) % LEVELS
    near = ((dst - src) % LEVELS == 1) | ((src - dst) % LEVELS == 1)
    full = (dst == heavy) | near
    out = jnp.where(full, LCAP, base)
    return jnp.where(src == dst, 0, out).astype(jnp.int32)


def with_ends(drawn, own_key, smallest, top_value):
    spot = [jax.random.randint(jax.random.fold_in(own_key, axis), (), 0, length) for axis, length in enumerate(drawn.shape)]
    widest = drawn.shape.index(max(drawn.shape))
    next_to = spot[:widest] + [(spot[widest] + 1) % drawn.shape[widest]] + spot[widest + 1:]
    return drawn.at[tuple(spot)].set(smallest).at[tuple(next_to)].set(top_value)


def block_levels(key, shape, cuts, smallest, top_value):
    def one(position, parts):
        steps = jax.random.uniform(jax.random.fold_in(jax.random.fold_in(key, 6), position), (parts,), jnp.float32, smallest / len(cuts), top_value / len(cuts))
        return jnp.repeat(jnp.exp(steps), shape[position] // parts).reshape((-1,) + (1,) * (len(shape) - position - 1))

    loudness = one(*cuts[0])
    for cut in cuts[1:]:
        loudness = loudness * one(*cut)
    return loudness


def centred(rng, dims, deviation, reach, cuts=(), dtype=jnp.bfloat16):
    result = deviation * jax.random.normal(rng, dims, jnp.float32)
    if cuts:
        result = result * block_levels(rng, dims, cuts, -0.22, 0.18)
    return jnp.clip(result, -reach, reach).astype(dtype)


def setup_inputs(seed: int = 0) -> dict:
    splits = jax.random.split(jax.random.key(seed), 12)
    fields = centred(splits[0], (LEVELS, BLOCKS, COMP, CELLS), 1.0, 6.0, ((0, 4), (1, 8)), jnp.float32)
    own_src = with_ends(jax.random.randint(splits[1], (LEVELS, BLOCKS), 0, BLK_DEV), jax.random.fold_in(splits[1], 1), 0, BLK_DEV - 1).astype(jnp.int32)
    own_weight = draw_own_weight(jax.random.fold_in(splits[11], 71), 0)
    send_block = with_ends(jax.random.randint(splits[3], (LEVELS, PEERS, PEERS, CAP), 0, BLK_DEV), jax.random.fold_in(splits[3], 1), 0, BLK_DEV - 1).astype(jnp.int32)
    send_target = with_ends(jax.random.randint(splits[4], (LEVELS, PEERS, PEERS, CAP), 0, BLK_DEV), jax.random.fold_in(splits[4], 1), 0, BLK_DEV - 1).astype(jnp.int32)
    send_count = draw_send_count(jax.random.fold_in(splits[11], 71), 0)
    send_weight = draw_send_weight(jax.random.fold_in(splits[11], 71), 0)
    left_block = with_ends(jax.random.randint(splits[7], (LEVELS, PEERS, LEVELS, LCAP), 0, BLK_DEV), jax.random.fold_in(splits[7], 1), 0, BLK_DEV - 1).astype(jnp.int32)
    left_target = with_ends(jax.random.randint(splits[8], (LEVELS, PEERS, LEVELS, LCAP), 0, BLK_DEV), jax.random.fold_in(splits[8], 1), 0, BLK_DEV - 1).astype(jnp.int32)
    left_count = draw_left_count(jax.random.fold_in(splits[11], 71), 0)
    left_weight = draw_left_weight(jax.random.fold_in(splits[11], 71), 0)
    return dict(fields=fields, own_src=own_src, own_weight=own_weight, send_block=send_block, send_target=send_target, send_count=send_count, send_weight=send_weight, left_block=left_block, left_target=left_target, left_count=left_count, left_weight=left_weight)


def reference(fields, own_src, own_weight, send_block, send_target, send_count, send_weight, left_block, left_target, left_count, left_weight):
    levels = fields.shape[0]
    peers = send_count.shape[1]
    blocks = fields.shape[1] // peers
    comp = fields.shape[2]
    cells = fields.shape[3]
    rounded = fields.astype(jnp.bfloat16).reshape(levels, peers, blocks, comp, cells)
    highest = lax.Precision.HIGHEST

    own_index = own_src.reshape(levels, peers, blocks, 1, 1).astype(jnp.int32)
    own_donor = jnp.take_along_axis(rounded, own_index, axis=2).astype(jnp.float32)
    own_frac = own_weight.reshape(levels, peers, blocks, cells, cells).astype(jnp.float32)
    own = jnp.einsum("lqbmk,lqbki->lqbmi", own_donor, own_frac, precision=highest)

    source_dev = lax.broadcasted_iota(jnp.int32, (peers, 1, 1), 0)
    recv_dev = lax.broadcasted_iota(jnp.int32, (1, peers, 1), 1)
    slot_cap = send_block.shape[3]

    def level_intra(packed):
        flds, blk, tgt, cnt, wts = packed
        donors = flds[source_dev, blk]
        valid = lax.broadcasted_iota(jnp.int32, (1, 1, slot_cap), 2) < cnt[:, :, None]
        donors = jnp.where(valid[..., None, None], donors, jnp.zeros_like(donors))
        contrib = jnp.einsum("spcmk,spcki->spcmi", donors.astype(jnp.float32), wts.astype(jnp.float32), precision=highest)
        receive = (recv_dev * blocks + tgt).reshape(-1).astype(jnp.int32)
        total = jnp.zeros((peers * blocks, comp, cells), jnp.float32)
        return total.at[receive].add(contrib.reshape(-1, comp, cells)).reshape(peers, blocks, comp, cells)

    intra = lax.map(level_intra, (rounded, send_block, send_target, send_count, send_weight))

    left_cap = left_block.shape[3]
    dev_index = lax.broadcasted_iota(jnp.int32, (peers, 1, 1), 0)

    def level_left(packed):
        flds, blk, cnt, wts = packed
        donors = flds[dev_index, blk]
        valid = lax.broadcasted_iota(jnp.int32, (1, 1, left_cap), 2) < cnt[:, :, None]
        donors = jnp.where(valid[..., None, None], donors, jnp.zeros_like(donors))
        return jnp.einsum("qlcmk,qlcki->qlcmi", donors.astype(jnp.float32), wts.astype(jnp.float32), precision=highest)

    left_terms = lax.map(level_left, (rounded, left_block, left_count, left_weight))
    dst_level = lax.broadcasted_iota(jnp.int32, (1, 1, levels, 1), 2)
    dev_here = lax.broadcasted_iota(jnp.int32, (1, peers, 1, 1), 1)
    recv_left = ((dst_level * peers + dev_here) * blocks + left_target).reshape(-1).astype(jnp.int32)
    leftover = jnp.zeros((levels * peers * blocks, comp, cells), jnp.float32)
    leftover = leftover.at[recv_left].add(left_terms.reshape(-1, comp, cells))
    leftover = leftover.reshape(levels, peers, blocks, comp, cells)

    remapped = (own + intra + leftover).reshape(levels, peers * blocks, comp, cells)
    totals = jnp.sum(remapped, axis=(0, 1, 3)) / (CELLS * BLK_DEV)
    return remapped, totals
```

```python
import functools

import jax
import jax.numpy as jnp
from jax import lax
from jax.experimental import pallas as pl
from jax.experimental.pallas import tpu as pltpu
from jax.sharding import PartitionSpec as P

MESH = pl.DeviceIdType.MESH
F32 = jnp.float32
BF16 = jnp.bfloat16
CHUNKS = 4


def kernel(
    nd,
    nl,
    direct,
    own_src_hbm,
    send_block_hbm,
    send_target_hbm,
    send_count_hbm,
    left_block_hbm,
    left_target_hbm,
    left_count_hbm,
    fields_hbm,
    own_hbm,
    send_hbm,
    left_hbm,
    out_ref,
    tot_ref,
    own_src,
    send_block,
    send_target,
    send_count,
    left_block,
    left_target,
    left_count,
    fields,
    own_w,
    send_w,
    left_w,
    load_sem,
    sbuf,
    rbuf,
    lsbuf,
    lrbuf,
    tbuf,
    trecv,
    urecv,
    move_sem,
):
    dev = lax.axis_index("dev")
    lvl = lax.axis_index("level")
    blocks, cells = own_w.shape[:2]
    comp = fields.shape[0] // blocks
    cap = send_w.shape[1]
    lcap = left_w.shape[1]
    rows = sbuf.shape[1] // cap
    per = blocks // CHUNKS

    barrier = pltpu.get_barrier_semaphore()
    left_peers = [lax.rem(lvl + r, nl) for r in range(1, nl)]
    send_peers = [lax.rem(dev + r, nd) for r in range(1, nd)]

    def load(src, dst, i):
        copy = pltpu.make_async_copy(src, dst, load_sem.at[i])
        copy.start()
        return copy

    small = [
        load(src, dst, i)
        for i, (src, dst) in enumerate(
            (
                (left_block_hbm, left_block),
                (left_target_hbm, left_target),
                (left_count_hbm, left_count),
                (send_block_hbm, send_block),
                (send_target_hbm, send_target),
                (send_count_hbm, send_count),
                (own_src_hbm, own_src),
                (fields_hbm, fields),
            )
        )
    ]
    n = len(small)
    for i, p in enumerate(left_peers):
        load(left_hbm.at[p], left_w.at[i], n)
    for i, p in enumerate(send_peers):
        load(send_hbm.at[p], send_w.at[i], n + 1)
    owns = [
        load(own_hbm.at[i * per : (i + 1) * per], own_w.at[i * per : (i + 1) * per], n + 2 + i)
        for i in range(CHUNKS)
    ]

    def peer_of(l, r):
        return {"level": lax.rem(lvl + l, nl), "dev": lax.rem(dev + r, nd)}

    offsets = [
        (l, r)
        for l in range(nl)
        for r in range(nd)
        if (l or r) and (direct or not (l and r))
    ]
    for l, r in offsets:
        pl.semaphore_signal(barrier, inc=1, device_id=peer_of(l, r), device_id_type=MESH)

    part = jnp.zeros((comp, cells), F32)

    def donor(index):
        return fields[pl.ds(index, comp, stride=blocks), :]

    def product(block, weight):
        return jnp.dot(block.astype(BF16), weight, preferred_element_type=F32)

    def message(buf, i, c, slot_block, slot_target, slot_count, weights, peer):
        block = donor(slot_block[c, peer])
        block = jnp.where(c < slot_count[0, peer], block, jnp.zeros_like(block))
        term = product(block, weights[i, c])
        target = jnp.full((rows - comp, cells), slot_target[c, peer].astype(F32), F32)
        buf[i, c * rows : (c + 1) * rows, :] = jnp.concatenate([term, target], axis=0).astype(BF16)
        return term

    def settle(ref, sem):
        pltpu.make_async_copy(ref, ref, sem).wait()

    for copy in small:
        copy.wait()
    settle(left_w, load_sem.at[n])
    for i, peer in enumerate(left_peers):
        for c in range(lcap):
            part += message(lsbuf, i, c, left_block, left_target, left_count, left_w, peer)
    settle(send_w, load_sem.at[n + 1])
    for i, peer in enumerate(send_peers):
        for c in range(cap):
            part += message(sbuf, i, c, send_block, send_target, send_count, send_w, peer)
    acc = []
    for b in range(blocks):
        if b % per == 0:
            owns[b // per].wait()
        term = product(donor(own_src[0, b]), own_w[b])
        part += term
        acc.append(term)

    sums = jnp.sum(part, axis=1, keepdims=True)
    same = lax.broadcasted_iota(jnp.int32, (comp, cells), 0) == lax.broadcasted_iota(
        jnp.int32, (comp, cells), 1
    )
    row = jnp.sum(jnp.where(same, sums, 0.0), axis=0, keepdims=True)
    tbuf[0] = row

    pl.semaphore_wait(barrier, len(offsets))

    def send(src, dst, s, who):
        pltpu.make_async_remote_copy(
            src_ref=src,
            dst_ref=dst,
            send_sem=move_sem.at[2 * s],
            recv_sem=move_sem.at[2 * s + 1],
            device_id=who,
            device_id_type=MESH,
        ).start()

    if direct:
        for i, (l, r) in enumerate(offsets):
            send(tbuf.at[0], urecv.at[i], 0, peer_of(l, r))
    else:
        for r in range(1, nd):
            send(tbuf.at[0], trecv.at[r - 1], 3, peer_of(0, r))
    for r in range(1, nl):
        send(lsbuf.at[r - 1], lrbuf.at[r - 1], 1, peer_of(r, 0))
    for r in range(1, nd):
        send(sbuf.at[r - 1], rbuf.at[r - 1], 2, peer_of(0, r))
    if not direct:
        settle(trecv, move_sem.at[7])
        row = row + jnp.sum(trecv[...], axis=0)
        tbuf[1] = row
        for r in range(1, nl):
            send(tbuf.at[1], urecv.at[r - 1], 0, peer_of(r, 0))

    def place(buf, i, slots):
        for c in range(slots):
            got = buf[i, c * rows : (c + 1) * rows, :].astype(F32)
            term = got[:comp]
            target = jnp.broadcast_to(got[comp : comp + 1], (comp, cells))
            for b in range(blocks):
                acc[b] = acc[b] + jnp.where(target == float(b), term, 0.0)

    settle(rbuf, move_sem.at[5])
    for i in range(nd - 1):
        place(rbuf, i, cap)
    settle(lrbuf, move_sem.at[3])
    for i in range(nl - 1):
        place(lrbuf, i, lcap)
    for b in range(blocks):
        out_ref[pl.ds(b, comp, stride=blocks), :] = acc[b]
    settle(sbuf, move_sem.at[4])
    settle(lsbuf, move_sem.at[2])
    settle(urecv, move_sem.at[0])
    if not direct:
        settle(trecv, move_sem.at[6])
    settle(urecv, move_sem.at[1])
    terms = [row] + [urecv[i] for i in range(urecv.shape[0])]
    while len(terms) > 1:
        half = len(terms) // 2
        terms = [a + b for a, b in zip(terms[:half], terms[half:])] + terms[2 * half :]
    tot_ref[...] = (terms[0] / (cells * blocks))[0, :comp]


def finish(remapped_vmem, totals_vmem, remapped_hbm, totals_hbm, sem):
    copies = [
        pltpu.make_async_copy(remapped_vmem, remapped_hbm, sem.at[0]),
        pltpu.make_async_copy(totals_vmem, totals_hbm, sem.at[1]),
    ]
    for copy in copies:
        copy.start()
    for copy in copies:
        copy.wait()


def solution(mesh):
    nd = mesh.shape["dev"]
    nl = mesh.shape["level"]
    direct = nd * nl <= 64
    last = (nd * nl if direct else nl) - 1

    def body(
        fields,
        own_src,
        own_weight,
        send_block,
        send_target,
        send_count,
        send_weight,
        left_block,
        left_target,
        left_count,
        left_weight,
    ):
        blocks, comp, cells = fields.shape[1:]
        cap = send_weight.shape[3]
        lcap = left_weight.shape[3]
        rows = -(-(comp + 1) // 16) * 16
        smem = functools.partial(pltpu.SMEM, dtype=jnp.int32)
        hbm = pl.BlockSpec(memory_space=pl.ANY)
        vmem = pl.BlockSpec(memory_space=pltpu.VMEM)
        dma = pltpu.SemaphoreType.DMA
        remapped, totals = pl.pallas_call(
            functools.partial(kernel, nd, nl, direct),
            out_shape=(
                pltpu.VMEM((comp * blocks, cells), F32),
                pltpu.VMEM((comp,), F32),
            ),
            in_specs=[hbm] * 11,
            out_specs=(vmem, vmem),
            scratch_shapes=[
                smem((1, blocks)),
                smem((cap, nd)),
                smem((cap, nd)),
                smem((1, nd)),
                smem((lcap, nl)),
                smem((lcap, nl)),
                smem((1, nl)),
                pltpu.VMEM((comp * blocks, cells), F32),
                pltpu.VMEM((blocks, cells, cells), BF16),
                pltpu.VMEM((nd - 1, cap, cells, cells), BF16),
                pltpu.VMEM((nl - 1, lcap, cells, cells), BF16),
                dma((10 + CHUNKS,)),
                pltpu.VMEM((nd - 1, cap * rows, cells), BF16),
                pltpu.VMEM((nd - 1, cap * rows, cells), BF16),
                pltpu.VMEM((nl - 1, lcap * rows, cells), BF16),
                pltpu.VMEM((nl - 1, lcap * rows, cells), BF16),
                pltpu.VMEM((2, 1, cells), F32),
                pltpu.VMEM((nd - 1, 1, cells), F32),
                pltpu.VMEM((last, 1, cells), F32),
                dma((6 if direct else 8,)),
            ],
            compiler_params=pltpu.CompilerParams(collective_id=0, has_side_effects=True),
        )(
            own_src,
            send_block[0, 0].T,
            send_target[0, 0].T,
            send_count[0],
            left_block[0, 0].T,
            left_target[0, 0].T,
            left_count[0],
            fields[0].transpose(1, 0, 2).reshape(comp * blocks, cells),
            own_weight[0],
            send_weight[0, 0],
            left_weight[0, 0],
        )
        remapped, totals = pl.pallas_call(
            finish,
            out_shape=(
                jax.ShapeDtypeStruct((comp * blocks, cells), F32),
                jax.ShapeDtypeStruct((comp,), F32),
            ),
            in_specs=[vmem, vmem],
            out_specs=(hbm, hbm),
            scratch_shapes=[dma((2,))],
        )(
            pltpu.with_memory_space_constraint(remapped, pltpu.VMEM),
            pltpu.with_memory_space_constraint(totals, pltpu.VMEM),
        )
        remapped = remapped.reshape(comp, blocks, cells).transpose(1, 0, 2)
        return remapped[None], totals

    in_specs = (
        P("level", "dev", None, None),
        P("level", "dev"),
        P("level", "dev", None, None),
        P("level", "dev", None, None),
        P("level", "dev", None, None),
        P("level", "dev", None),
        P("level", "dev", None, None, None, None),
        P("level", "dev", None, None),
        P("level", "dev", None, None),
        P("level", "dev", None),
        P("level", "dev", None, None, None, None),
    )
    out_specs = (P("level", "dev", None, None), P())
    return jax.shard_map(body, mesh=mesh, in_specs=in_specs, out_specs=out_specs, check_vma=False)
```

```python
import functools

import jax
import jax.numpy as jnp
from jax import lax
from jax.experimental import pallas as pl
from jax.experimental.pallas import tpu as pltpu
from jax.sharding import PartitionSpec as P

MESH = pl.DeviceIdType.MESH
F32 = jnp.float32
BF16 = jnp.bfloat16
CHUNKS = 1


def tree(terms):
    while len(terms) > 1:
        half = len(terms) // 2
        terms = [a + b for a, b in zip(terms[:half], terms[half:])] + terms[2 * half :]
    return terms[0]


def kernel(
    nd,
    nl,
    direct,
    own_src_hbm,
    send_block_hbm,
    send_target_hbm,
    send_count_hbm,
    left_block_hbm,
    left_target_hbm,
    left_count_hbm,
    fields_hbm,
    own_hbm,
    send_hbm,
    left_hbm,
    out_ref,
    tot_ref,
    own_src,
    send_block,
    send_target,
    send_count,
    left_block,
    left_target,
    left_count,
    fields,
    donors,
    own_w,
    send_w,
    left_w,
    sbuf,
    rbuf,
    lsbuf,
    lrbuf,
    tbuf,
    trecv,
    urecv,
    recv_sem,
):
    dev = lax.axis_index("dev")
    lvl = lax.axis_index("level")
    blocks, rows, cells = donors.shape
    comp = fields.shape[0] // blocks
    cap = send_w.shape[1]
    lcap = left_w.shape[1]
    per = blocks // CHUNKS

    barrier = pltpu.get_barrier_semaphore()
    left_peers = [lax.rem(lvl + r, nl) for r in range(1, nl)]
    send_peers = [lax.rem(dev + r, nd) for r in range(1, nd)]

    def settle(ref, sem):
        pltpu.make_async_copy(ref, ref, sem).wait()

    def peer_of(l, r):
        return {"level": lax.rem(lvl + l, nl), "dev": lax.rem(dev + r, nd)}

    offsets = [
        (l, r)
        for l in (*range(1, nl), 0)
        for r in (1, 2, 0, *range(3, nd))
        if (l or r) and (direct or not (l and r))
    ]

    def run(load_sem, send_sem):
        def load(src, dst, i):
            copy = pltpu.make_async_copy(src, dst, load_sem.at[i])
            copy.start()
            return copy

        small = [
            load(src, dst, i)
            for i, (src, dst) in enumerate(
                (
                    (fields_hbm, fields),
                    (left_block_hbm, left_block),
                    (left_target_hbm, left_target),
                    (left_count_hbm, left_count),
                    (send_block_hbm, send_block),
                    (send_target_hbm, send_target),
                    (send_count_hbm, send_count),
                    (own_src_hbm, own_src),
                )
            )
        ]
        n = len(small)
        owns = [
            load(own_hbm.at[i * per : (i + 1) * per], own_w.at[i * per : (i + 1) * per], n + 2 + i)
            for i in range(CHUNKS)
        ]

        for i, p in enumerate(send_peers):
            load(send_hbm.at[p], send_w.at[i], n + 1)
        for i, p in enumerate(left_peers):
            load(left_hbm.at[p], left_w.at[i], n)

        for l, r in offsets:
            pl.semaphore_signal(barrier, inc=1, device_id=peer_of(l, r), device_id_type=MESH)

        def products(pairs):
            terms = []
            for i in range(0, len(pairs), 2):
                group = pairs[i : i + 2]
                left = jnp.concatenate([block for block, _ in group], axis=0)
                right = jnp.concatenate([weight for _, weight in group], axis=1)
                both = jnp.dot(left, right, preferred_element_type=F32)
                for j in range(len(group)):
                    terms.append(both[j * rows : (j + 1) * rows, j * cells : (j + 1) * cells])
            return terms

        line = lax.broadcasted_iota(jnp.int32, (rows, cells), 0)

        held = []

        def messages(buf, slots, slot_block, slot_target, slot_count, weights, peers):
            keys = [(i, c, p) for i, p in enumerate(peers) for c in range(slots)]
            pairs = []
            for i, c, p in keys:
                block = donors[slot_block[c, p]]
                block = jnp.where(c < slot_count[0, p], block, jnp.zeros_like(block))
                pairs.append((block, weights[i, c]))
            terms = products(pairs)
            held.append((buf, slot_target, keys, terms))
            return terms

        def fill():
            for buf, slot_target, keys, terms in held:
                for (i, c, p), term in zip(keys, terms):
                    filled = jnp.where(line < comp, term, slot_target[c, p].astype(F32))
                    buf[i, c * rows : (c + 1) * rows, :] = filled.astype(BF16)

        small[0].wait()
        for b in range(blocks):
            block = fields[pl.ds(b, comp, stride=blocks), :]
            block = jnp.concatenate([block, jnp.zeros((rows - comp, cells), F32)], axis=0)
            donors[b] = block.astype(BF16)
        for copy in small[1:]:
            copy.wait()
        sent = []
        acc = []
        for i in range(CHUNKS):
            owns[i].wait()
            acc += products([(donors[own_src[0, b]], own_w[b]) for b in range(i * per, (i + 1) * per)])

        settle(send_w, load_sem.at[n + 1])
        settle(left_w, load_sem.at[n])
        sent += messages(sbuf, cap, send_block, send_target, send_count, send_w, send_peers)
        sent += messages(lsbuf, lcap, left_block, left_target, left_count, left_w, left_peers)
        part = tree(sent + acc)
        sums = jnp.sum(part, axis=1, keepdims=True)
        same = line == lax.broadcasted_iota(jnp.int32, (rows, cells), 1)
        row = jnp.sum(jnp.where(same, sums, 0.0), axis=0, keepdims=True)
        tbuf[0] = row

        pl.semaphore_wait(barrier, len(offsets))

        def send(src, dst, s, who):
            pltpu.make_async_remote_copy(
                src_ref=src,
                dst_ref=dst,
                send_sem=send_sem.at[s],
                recv_sem=recv_sem.at[s],
                device_id=who,
                device_id_type=MESH,
            ).start()

        if direct:
            for i, (l, r) in enumerate(offsets):
                send(tbuf.at[0], urecv.at[i], 0, peer_of(l, r))
        else:
            for r in range(1, nd):
                send(tbuf.at[0], trecv.at[r - 1], 3, peer_of(0, r))
        fill()
        for r in range(1, nl):
            send(lsbuf.at[r - 1], lrbuf.at[r - 1], 1, peer_of(r, 0))
        for r in range(1, nd):
            send(sbuf.at[r - 1], rbuf.at[r - 1], 2, peer_of(0, r))
        if not direct:
            settle(trecv, recv_sem.at[3])
            row = row + jnp.sum(trecv[...], axis=0)
            tbuf[1] = row
            for r in range(1, nl):
                send(tbuf.at[1], urecv.at[r - 1], 0, peer_of(r, 0))

        acc = [term[:comp] for term in acc]

        def place(buf, i, slots):
            for c in range(slots):
                got = buf[i, c * rows : (c + 1) * rows, :].astype(F32)
                term = got[:comp]
                target = jnp.broadcast_to(got[comp : comp + 1], (comp, cells))
                for b in range(blocks):
                    acc[b] = acc[b] + jnp.where(target == float(b), term, 0.0)

        settle(rbuf, recv_sem.at[2])
        for i in range(nd - 1):
            place(rbuf, i, cap)
        settle(lrbuf, recv_sem.at[1])
        for i in range(nl - 1):
            place(lrbuf, i, lcap)
        for b in range(blocks):
            out_ref[pl.ds(b, comp, stride=blocks), :] = acc[b]
        settle(sbuf, send_sem.at[2])
        settle(lsbuf, send_sem.at[1])
        settle(urecv, send_sem.at[0])
        if not direct:
            settle(trecv, send_sem.at[3])

    pl.run_scoped(
        run, pltpu.SemaphoreType.DMA((10 + CHUNKS,)), pltpu.SemaphoreType.DMA((recv_sem.shape[0],))
    )
    settle(urecv, recv_sem.at[0])
    mine = tbuf[0 if direct else 1]
    total = tree([mine] + [urecv[i] for i in range(urecv.shape[0])])
    tot_ref[...] = (total / (cells * blocks))[0, :comp]


def finish(remapped_vmem, totals_vmem, remapped_hbm, totals_hbm):
    def run(sem):
        copies = [
            pltpu.make_async_copy(remapped_vmem, remapped_hbm, sem.at[0]),
            pltpu.make_async_copy(totals_vmem, totals_hbm, sem.at[1]),
        ]
        for copy in copies:
            copy.start()
        for copy in copies:
            copy.wait()

    pl.run_scoped(run, pltpu.SemaphoreType.DMA((2,)))


def solution(mesh):
    nd = mesh.shape["dev"]
    nl = mesh.shape["level"]
    direct = nd * nl <= 64
    last = (nd * nl if direct else nl) - 1

    def body(
        fields,
        own_src,
        own_weight,
        send_block,
        send_target,
        send_count,
        send_weight,
        left_block,
        left_target,
        left_count,
        left_weight,
    ):
        blocks, comp, cells = fields.shape[1:]
        cap = send_weight.shape[3]
        lcap = left_weight.shape[3]
        rows = -(-(comp + 1) // 16) * 16
        smem = functools.partial(pltpu.SMEM, dtype=jnp.int32)
        hbm = pl.BlockSpec(memory_space=pl.ANY)
        vmem = pl.BlockSpec(memory_space=pltpu.VMEM)
        dma = pltpu.SemaphoreType.DMA
        remapped, totals = pl.pallas_call(
            functools.partial(kernel, nd, nl, direct),
            out_shape=(
                pltpu.VMEM((comp * blocks, cells), F32),
                pltpu.VMEM((comp,), F32),
            ),
            in_specs=[hbm] * 11,
            out_specs=(vmem, vmem),
            scratch_shapes=[
                smem((1, blocks)),
                smem((cap, nd)),
                smem((cap, nd)),
                smem((1, nd)),
                smem((lcap, nl)),
                smem((lcap, nl)),
                smem((1, nl)),
                pltpu.VMEM((comp * blocks, cells), F32),
                pltpu.VMEM((blocks, rows, cells), BF16),
                pltpu.VMEM((blocks, cells, cells), BF16),
                pltpu.VMEM((nd - 1, cap, cells, cells), BF16),
                pltpu.VMEM((nl - 1, lcap, cells, cells), BF16),
                pltpu.VMEM((nd - 1, cap * rows, cells), BF16),
                pltpu.VMEM((nd - 1, cap * rows, cells), BF16),
                pltpu.VMEM((nl - 1, lcap * rows, cells), BF16),
                pltpu.VMEM((nl - 1, lcap * rows, cells), BF16),
                pltpu.VMEM((2, 1, cells), F32),
                pltpu.VMEM((nd - 1, 1, cells), F32),
                pltpu.VMEM((last, 1, cells), F32),
                dma((3 if direct else 4,)),
            ],
            compiler_params=pltpu.CompilerParams(collective_id=0, has_side_effects=True),
        )(
            own_src,
            send_block[0, 0].T,
            send_target[0, 0].T,
            send_count[0],
            left_block[0, 0].T,
            left_target[0, 0].T,
            left_count[0],
            fields[0].transpose(1, 0, 2).reshape(comp * blocks, cells),
            own_weight[0],
            send_weight[0, 0],
            left_weight[0, 0],
        )
        remapped, totals = pl.pallas_call(
            finish,
            out_shape=(
                jax.ShapeDtypeStruct((comp * blocks, cells), F32),
                jax.ShapeDtypeStruct((comp,), F32),
            ),
            in_specs=[vmem, vmem],
            out_specs=(hbm, hbm),
        )(
            pltpu.with_memory_space_constraint(remapped, pltpu.VMEM),
            pltpu.with_memory_space_constraint(totals, pltpu.VMEM),
        )
        remapped = remapped.reshape(comp, blocks, cells).transpose(1, 0, 2)
        return remapped[None], totals

    in_specs = (
        P("level", "dev", None, None),
        P("level", "dev"),
        P("level", "dev", None, None),
        P("level", "dev", None, None),
        P("level", "dev", None, None),
        P("level", "dev", None),
        P("level", "dev", None, None, None, None),
        P("level", "dev", None, None),
        P("level", "dev", None, None),
        P("level", "dev", None),
        P("level", "dev", None, None, None, None),
    )
    out_specs = (P("level", "dev", None, None), P())
    return jax.shard_map(body, mesh=mesh, in_specs=in_specs, out_specs=out_specs, check_vma=False)
```

```python
import functools

import jax
import jax.numpy as jnp
from jax import lax
from jax.experimental import pallas as pl
from jax.experimental.pallas import tpu as pltpu
from jax.sharding import PartitionSpec as P

MESH = pl.DeviceIdType.MESH
F32 = jnp.float32
BF16 = jnp.bfloat16


def tree(terms):
    while len(terms) > 1:
        half = len(terms) // 2
        terms = [a + b for a, b in zip(terms[:half], terms[half:])] + terms[2 * half :]
    return terms[0]


def kernel(
    nd,
    nl,
    direct,
    own_src_hbm,
    send_block_hbm,
    send_target_hbm,
    send_count_hbm,
    left_block_hbm,
    left_target_hbm,
    left_count_hbm,
    fields_hbm,
    own_hbm,
    send_hbm,
    left_hbm,
    out_ref,
    tot_ref,
    own_src,
    send_block,
    send_target,
    send_count,
    left_block,
    left_target,
    left_count,
    fields,
    donors,
    own_w,
    send_w,
    left_w,
    sbuf,
    rbuf,
    lsbuf,
    lrbuf,
    tbuf,
    trecv,
    urecv,
    recv_sem,
):
    dev = lax.axis_index("dev")
    lvl = lax.axis_index("level")
    blocks, rows, cells = donors.shape
    comp = fields.shape[0] // blocks
    cap = send_w.shape[1]
    lcap = left_w.shape[1]
    early = nd // 2

    barrier = pltpu.get_barrier_semaphore()
    left_peers = [lax.rem(lvl + r, nl) for r in range(1, nl)]
    send_peers = [lax.rem(dev + r, nd) for r in range(1, nd)]

    def settle(ref, sem):
        pltpu.make_async_copy(ref, ref, sem).wait()

    def peer_of(l, r):
        return {"level": lax.rem(lvl + l, nl), "dev": lax.rem(dev + r, nd)}

    offsets = [
        (l, r)
        for l in (*range(1, nl), 0)
        for r in (*reversed(range(min(3, nd))), *range(3, nd))
        if (l or r) and (direct or not (l and r))
    ]

    def run(load_sem, send_sem):
        def load(src, dst, i):
            copy = pltpu.make_async_copy(src, dst, load_sem.at[i])
            copy.start()
            return copy

        small = [
            load(src, dst, i)
            for i, (src, dst) in enumerate(
                (
                    (fields_hbm, fields),
                    (left_block_hbm, left_block),
                    (left_target_hbm, left_target),
                    (left_count_hbm, left_count),
                    (send_block_hbm, send_block),
                    (send_target_hbm, send_target),
                    (send_count_hbm, send_count),
                    (own_src_hbm, own_src),
                )
            )
        ]
        n = len(small)
        owns = load(own_hbm, own_w, n + 3)
        for i, p in enumerate(send_peers):
            load(send_hbm.at[p], send_w.at[i], n + 1 if i < early else n + 2)
        for i, p in enumerate(left_peers):
            load(left_hbm.at[p], left_w.at[i], n)

        for l, r in offsets:
            pl.semaphore_signal(barrier, inc=1, device_id=peer_of(l, r), device_id_type=MESH)

        def products(pairs):
            terms = []
            for i in range(0, len(pairs), 2):
                group = pairs[i : i + 2]
                left = jnp.concatenate([block for block, _ in group], axis=0)
                right = jnp.concatenate([weight for _, weight in group], axis=1)
                both = jnp.dot(left, right, preferred_element_type=F32)
                for j in range(len(group)):
                    terms.append(both[j * rows : (j + 1) * rows, j * cells : (j + 1) * cells])
            return terms

        line = lax.broadcasted_iota(jnp.int32, (rows, cells), 0)

        send_slots = [(i, c, p) for i, p in enumerate(send_peers) for c in range(cap)]
        left_slots = [(i, c, p) for i, p in enumerate(left_peers) for c in range(lcap)]

        def gather(slots, slot_block, slot_count, weights):
            pairs = []
            for i, c, p in slots:
                block = donors[slot_block[c, p]]
                block = jnp.where(c < slot_count[0, p], block, jnp.zeros_like(block))
                pairs.append((block, weights[i, c]))
            return pairs

        def fill(buf, slots, slot_target, terms):
            for (i, c, p), term in zip(slots, terms):
                filled = jnp.where(line < comp, term, slot_target[c, p].astype(F32))
                buf[i, c * rows : (c + 1) * rows, :] = filled.astype(BF16)

        small[0].wait()
        for b in range(blocks):
            block = fields[pl.ds(b, comp, stride=blocks), :]
            block = jnp.concatenate([block, jnp.zeros((rows - comp, cells), F32)], axis=0)
            donors[b] = block.astype(BF16)
        for copy in small[1:]:
            copy.wait()
        owns.wait()
        settle(send_w.at[:early], load_sem.at[n + 1])
        cut = early * cap
        terms = products(
            [(donors[own_src[0, b]], own_w[b]) for b in range(blocks)]
            + gather(send_slots[:cut], send_block, send_count, send_w)
        )
        acc, sent = terms[:blocks], terms[blocks:]
        part = tree(terms)
        settle(send_w.at[early:], load_sem.at[n + 2])
        settle(left_w, load_sem.at[n])
        terms = products(
            gather(send_slots[cut:], send_block, send_count, send_w)
            + gather(left_slots, left_block, left_count, left_w)
        )
        sent += terms
        part += tree(terms)

        sums = jnp.sum(part, axis=1, keepdims=True)
        same = line == lax.broadcasted_iota(jnp.int32, (rows, cells), 1)
        row = jnp.sum(jnp.where(same, sums, 0.0), axis=0, keepdims=True)
        tbuf[0] = row

        pl.semaphore_wait(barrier, len(offsets))

        def send(src, dst, s, who):
            pltpu.make_async_remote_copy(
                src_ref=src,
                dst_ref=dst,
                send_sem=send_sem.at[s],
                recv_sem=recv_sem.at[s],
                device_id=who,
                device_id_type=MESH,
            ).start()

        if direct:
            for i, (l, r) in enumerate(offsets):
                send(tbuf.at[0], urecv.at[i], 0, peer_of(l, r))
        else:
            for r in range(1, nd):
                send(tbuf.at[0], trecv.at[r - 1], 3, peer_of(0, r))
        fill(sbuf, send_slots, send_target, sent[: len(send_slots)])
        fill(lsbuf, left_slots, left_target, sent[len(send_slots) :])
        for r in range(1, nl):
            send(lsbuf.at[r - 1], lrbuf.at[r - 1], 1, peer_of(r, 0))
        for r in range(1, nd):
            send(sbuf.at[r - 1], rbuf.at[r - 1], 2, peer_of(0, r))
        if not direct:
            settle(trecv, recv_sem.at[3])
            row = row + jnp.sum(trecv[...], axis=0)
            tbuf[1] = row
            for r in range(1, nl):
                send(tbuf.at[1], urecv.at[r - 1], 0, peer_of(r, 0))

        acc = [term[:comp] for term in acc]

        def place(buf, i, slots):
            for c in range(slots):
                got = buf[i, c * rows : (c + 1) * rows, :].astype(F32)
                term = got[:comp]
                target = jnp.broadcast_to(got[comp : comp + 1], (comp, cells))
                for b in range(blocks):
                    acc[b] = acc[b] + jnp.where(target == float(b), term, 0.0)

        settle(rbuf, recv_sem.at[2])
        for i in range(nd - 1):
            place(rbuf, i, cap)
        settle(lrbuf, recv_sem.at[1])
        for i in range(nl - 1):
            place(lrbuf, i, lcap)
        for b in range(blocks):
            out_ref[pl.ds(b, comp, stride=blocks), :] = acc[b]
        settle(sbuf, send_sem.at[2])
        settle(lsbuf, send_sem.at[1])
        settle(urecv, send_sem.at[0])
        if not direct:
            settle(trecv, send_sem.at[3])

    pl.run_scoped(
        run, pltpu.SemaphoreType.DMA((12,)), pltpu.SemaphoreType.DMA((recv_sem.shape[0],))
    )
    settle(urecv, recv_sem.at[0])
    mine = tbuf[0 if direct else 1]
    total = tree([mine] + [urecv[i] for i in range(urecv.shape[0])])
    tot_ref[...] = (total * (1.0 / (cells * blocks)))[0, :comp]


def finish(remapped_vmem, totals_vmem, remapped_hbm, totals_hbm):
    def run(sem):
        copies = [
            pltpu.make_async_copy(remapped_vmem, remapped_hbm, sem.at[0]),
            pltpu.make_async_copy(totals_vmem, totals_hbm, sem.at[1]),
        ]
        for copy in copies:
            copy.start()
        for copy in copies:
            copy.wait()

    pl.run_scoped(run, pltpu.SemaphoreType.DMA((2,)))


def solution(mesh):
    nd = mesh.shape["dev"]
    nl = mesh.shape["level"]
    direct = nd * nl <= 64
    last = (nd * nl if direct else nl) - 1

    def body(
        fields,
        own_src,
        own_weight,
        send_block,
        send_target,
        send_count,
        send_weight,
        left_block,
        left_target,
        left_count,
        left_weight,
    ):
        blocks, comp, cells = fields.shape[1:]
        cap = send_weight.shape[3]
        lcap = left_weight.shape[3]
        rows = -(-(comp + 1) // 16) * 16
        smem = functools.partial(pltpu.SMEM, dtype=jnp.int32)
        hbm = pl.BlockSpec(memory_space=pl.ANY)
        vmem = pl.BlockSpec(memory_space=pltpu.VMEM)
        dma = pltpu.SemaphoreType.DMA
        remapped, totals = pl.pallas_call(
            functools.partial(kernel, nd, nl, direct),
            out_shape=(
                pltpu.VMEM((comp * blocks, cells), F32),
                pltpu.VMEM((comp,), F32),
            ),
            in_specs=[hbm] * 11,
            out_specs=(vmem, vmem),
            scratch_shapes=[
                smem((1, blocks)),
                smem((cap, nd)),
                smem((cap, nd)),
                smem((1, nd)),
                smem((lcap, nl)),
                smem((lcap, nl)),
                smem((1, nl)),
                pltpu.VMEM((comp * blocks, cells), F32),
                pltpu.VMEM((blocks, rows, cells), BF16),
                pltpu.VMEM((blocks, cells, cells), BF16),
                pltpu.VMEM((nd - 1, cap, cells, cells), BF16),
                pltpu.VMEM((nl - 1, lcap, cells, cells), BF16),
                pltpu.VMEM((nd - 1, cap * rows, cells), BF16),
                pltpu.VMEM((nd - 1, cap * rows, cells), BF16),
                pltpu.VMEM((nl - 1, lcap * rows, cells), BF16),
                pltpu.VMEM((nl - 1, lcap * rows, cells), BF16),
                pltpu.VMEM((2, 1, cells), F32),
                pltpu.VMEM((nd - 1, 1, cells), F32),
                pltpu.VMEM((last, 1, cells), F32),
                dma((3 if direct else 4,)),
            ],
            compiler_params=pltpu.CompilerParams(collective_id=0, has_side_effects=True),
        )(
            own_src,
            send_block[0, 0].T,
            send_target[0, 0].T,
            send_count[0],
            left_block[0, 0].T,
            left_target[0, 0].T,
            left_count[0],
            fields[0].transpose(1, 0, 2).reshape(comp * blocks, cells),
            own_weight[0],
            send_weight[0, 0],
            left_weight[0, 0],
        )
        remapped, totals = pl.pallas_call(
            finish,
            out_shape=(
                jax.ShapeDtypeStruct((comp * blocks, cells), F32),
                jax.ShapeDtypeStruct((comp,), F32),
            ),
            in_specs=[vmem, vmem],
            out_specs=(hbm, hbm),
        )(
            pltpu.with_memory_space_constraint(remapped, pltpu.VMEM),
            pltpu.with_memory_space_constraint(totals, pltpu.VMEM),
        )
        remapped = remapped.reshape(comp, blocks, cells).transpose(1, 0, 2)
        return remapped[None], totals

    in_specs = (
        P("level", "dev", None, None),
        P("level", "dev"),
        P("level", "dev", None, None),
        P("level", "dev", None, None),
        P("level", "dev", None, None),
        P("level", "dev", None),
        P("level", "dev", None, None, None, None),
        P("level", "dev", None, None),
        P("level", "dev", None, None),
        P("level", "dev", None),
        P("level", "dev", None, None, None, None),
    )
    out_specs = (P("level", "dev", None, None), P())
    return jax.shard_map(body, mesh=mesh, in_specs=in_specs, out_specs=out_specs, check_vma=False)
```

```python
import functools

import jax
import jax.numpy as jnp
from jax import lax
from jax.experimental import pallas as pl
from jax.experimental.pallas import tpu as pltpu
from jax.sharding import PartitionSpec as P

MESH = pl.DeviceIdType.MESH
F32 = jnp.float32
BF16 = jnp.bfloat16


def tree(terms):
    while len(terms) > 1:
        half = len(terms) // 2
        terms = [a + b for a, b in zip(terms[:half], terms[half:])] + terms[2 * half :]
    return terms[0]


def kernel(
    nd,
    nl,
    direct,
    own_src_hbm,
    send_block_hbm,
    send_target_hbm,
    send_count_hbm,
    left_block_hbm,
    left_target_hbm,
    left_count_hbm,
    fields_hbm,
    own_hbm,
    send_hbm,
    left_hbm,
    out_ref,
    tot_ref,
    own_src,
    send_block,
    send_target,
    send_count,
    left_block,
    left_target,
    left_count,
    fields,
    donors,
    own_w,
    send_w,
    left_w,
    sbuf,
    rbuf,
    tbuf,
    trecv,
    urecv,
    recv_sem,
):
    dev = lax.axis_index("dev")
    lvl = lax.axis_index("level")
    blocks, rows, cells = donors.shape
    comp = fields.shape[0] // blocks
    cap = send_w.shape[1]
    lcap = left_w.shape[1]
    early = nd // 2
    base = (nd - 1) * cap

    barrier = pltpu.get_barrier_semaphore()
    left_peers = [lax.rem(lvl + r, nl) for r in range(1, nl)]
    send_peers = [lax.rem(dev + r, nd) for r in range(1, nd)]

    def settle(ref, sem):
        pltpu.make_async_copy(ref, ref, sem).wait()

    def peer_of(l, r):
        return {"level": lax.rem(lvl + l, nl), "dev": lax.rem(dev + r, nd)}

    offsets = [
        (l, r)
        for l in (*range(1, nl), 0)
        for r in (*reversed(range(min(3, nd))), *range(3, nd))
        if (l or r) and (direct or not (l and r))
    ]

    def run(load_sem, send_sem):
        def load(src, dst, i):
            copy = pltpu.make_async_copy(src, dst, load_sem.at[i])
            copy.start()
            return copy

        small = [
            load(src, dst, i)
            for i, (src, dst) in enumerate(
                (
                    (fields_hbm, fields),
                    (left_block_hbm, left_block),
                    (left_target_hbm, left_target),
                    (left_count_hbm, left_count),
                    (send_block_hbm, send_block),
                    (send_target_hbm, send_target),
                    (send_count_hbm, send_count),
                    (own_src_hbm, own_src),
                )
            )
        ]
        n = len(small)
        owns = load(own_hbm, own_w, n + 3)
        for i, p in enumerate(send_peers):
            load(send_hbm.at[p], send_w.at[i], n + 1 if i < early else n + 2)
        for i, p in enumerate(left_peers):
            load(left_hbm.at[p], left_w.at[i], n)

        for l, r in offsets:
            pl.semaphore_signal(barrier, inc=1, device_id=peer_of(l, r), device_id_type=MESH)

        def products(pairs):
            terms = []
            for i in range(0, len(pairs), 2):
                group = pairs[i : i + 2]
                left = jnp.concatenate([block for block, _ in group], axis=0)
                right = jnp.concatenate([weight for _, weight in group], axis=1)
                both = jnp.dot(left, right, preferred_element_type=F32)
                for j in range(len(group)):
                    terms.append(both[j * rows : (j + 1) * rows, j * cells : (j + 1) * cells])
            return terms

        line = lax.broadcasted_iota(jnp.int32, (rows, cells), 0)

        send_slots = [(i, c, p) for i, p in enumerate(send_peers) for c in range(cap)]
        left_slots = [(i, c, p) for i, p in enumerate(left_peers) for c in range(lcap)]

        def gather(slots, slot_block, slot_count, weights):
            pairs = []
            for i, c, p in slots:
                block = donors[slot_block[c, p]]
                block = jnp.where(c < slot_count[0, p], block, jnp.zeros_like(block))
                pairs.append((block, weights[i, c]))
            return pairs

        def fill(at, slots, slot_target, terms):
            for k, ((_, c, p), term) in enumerate(zip(slots, terms)):
                filled = jnp.where(line < comp, term, slot_target[c, p].astype(F32))
                sbuf[at + k] = filled.astype(BF16)

        small[0].wait()
        for b in range(blocks):
            block = fields[pl.ds(b, comp, stride=blocks), :]
            block = jnp.concatenate([block, jnp.zeros((rows - comp, cells), F32)], axis=0)
            donors[b] = block.astype(BF16)
        for copy in small[1:]:
            copy.wait()
        owns.wait()
        settle(send_w.at[:early], load_sem.at[n + 1])
        cut = early * cap
        terms = products(
            [(donors[own_src[0, b]], own_w[b]) for b in range(blocks)]
            + gather(send_slots[:cut], send_block, send_count, send_w)
        )
        acc, sent = terms[:blocks], terms[blocks:]
        part = tree(terms)
        settle(send_w.at[early:], load_sem.at[n + 2])
        settle(left_w, load_sem.at[n])
        terms = products(
            gather(send_slots[cut:], send_block, send_count, send_w)
            + gather(left_slots, left_block, left_count, left_w)
        )
        sent += terms
        part += tree(terms)

        sums = jnp.sum(part, axis=1, keepdims=True)
        same = line == lax.broadcasted_iota(jnp.int32, (rows, cells), 1)
        row = jnp.sum(jnp.where(same, sums, 0.0), axis=0, keepdims=True)
        tbuf[0] = row

        pl.semaphore_wait(barrier, len(offsets))

        def send(src, dst, s, who):
            pltpu.make_async_remote_copy(
                src_ref=src,
                dst_ref=dst,
                send_sem=send_sem.at[s],
                recv_sem=recv_sem.at[s],
                device_id=who,
                device_id_type=MESH,
            ).start()

        if direct:
            for i, (l, r) in enumerate(offsets):
                send(tbuf.at[0], urecv.at[i], 0, peer_of(l, r))
        else:
            for r in range(1, nd):
                send(tbuf.at[0], trecv.at[r - 1], 2, peer_of(0, r))
        fill(0, send_slots, send_target, sent[:base])
        fill(base, left_slots, left_target, sent[base:])
        for r in range(1, nl):
            part_of = pl.ds(base + (r - 1) * lcap, lcap)
            send(sbuf.at[part_of], rbuf.at[part_of], 1, peer_of(r, 0))
        for r in range(1, nd):
            part_of = pl.ds((r - 1) * cap, cap)
            send(sbuf.at[part_of], rbuf.at[part_of], 1, peer_of(0, r))
        if not direct:
            settle(trecv, recv_sem.at[2])
            row = row + jnp.sum(trecv[...], axis=0)
            tbuf[1] = row
            for r in range(1, nl):
                send(tbuf.at[1], urecv.at[r - 1], 0, peer_of(r, 0))

        acc = [term[:comp] for term in acc]

        settle(rbuf, recv_sem.at[1])
        for k in range(rbuf.shape[0]):
            got = rbuf[k].astype(F32)
            term = got[:comp]
            target = jnp.broadcast_to(got[comp : comp + 1], (comp, cells))
            for b in range(blocks):
                acc[b] = acc[b] + jnp.where(target == float(b), term, 0.0)
        for b in range(blocks):
            out_ref[pl.ds(b, comp, stride=blocks), :] = acc[b]
        settle(sbuf, send_sem.at[1])
        settle(urecv, send_sem.at[0])
        if not direct:
            settle(trecv, send_sem.at[2])

    pl.run_scoped(
        run, pltpu.SemaphoreType.DMA((12,)), pltpu.SemaphoreType.DMA((recv_sem.shape[0],))
    )
    settle(urecv, recv_sem.at[0])
    mine = tbuf[0 if direct else 1]
    total = tree([mine] + [urecv[i] for i in range(urecv.shape[0])])
    tot_ref[...] = (total * (1.0 / (cells * blocks)))[0, :comp]


def finish(remapped_vmem, totals_vmem, remapped_hbm, totals_hbm):
    def run(sem):
        copies = [
            pltpu.make_async_copy(remapped_vmem, remapped_hbm, sem.at[0]),
            pltpu.make_async_copy(totals_vmem, totals_hbm, sem.at[1]),
        ]
        for copy in copies:
            copy.start()
        for copy in copies:
            copy.wait()

    pl.run_scoped(run, pltpu.SemaphoreType.DMA((2,)))


def solution(mesh):
    nd = mesh.shape["dev"]
    nl = mesh.shape["level"]
    direct = nd * nl <= 64
    last = (nd * nl if direct else nl) - 1

    def body(
        fields,
        own_src,
        own_weight,
        send_block,
        send_target,
        send_count,
        send_weight,
        left_block,
        left_target,
        left_count,
        left_weight,
    ):
        blocks, comp, cells = fields.shape[1:]
        cap = send_weight.shape[3]
        lcap = left_weight.shape[3]
        rows = -(-(comp + 1) // 16) * 16
        smem = functools.partial(pltpu.SMEM, dtype=jnp.int32)
        hbm = pl.BlockSpec(memory_space=pl.ANY)
        vmem = pl.BlockSpec(memory_space=pltpu.VMEM)
        dma = pltpu.SemaphoreType.DMA
        remapped, totals = pl.pallas_call(
            functools.partial(kernel, nd, nl, direct),
            out_shape=(
                pltpu.VMEM((comp * blocks, cells), F32),
                pltpu.VMEM((comp,), F32),
            ),
            in_specs=[hbm] * 11,
            out_specs=(vmem, vmem),
            scratch_shapes=[
                smem((1, blocks)),
                smem((cap, nd)),
                smem((cap, nd)),
                smem((1, nd)),
                smem((lcap, nl)),
                smem((lcap, nl)),
                smem((1, nl)),
                pltpu.VMEM((comp * blocks, cells), F32),
                pltpu.VMEM((blocks, rows, cells), BF16),
                pltpu.VMEM((blocks, cells, cells), BF16),
                pltpu.VMEM((nd - 1, cap, cells, cells), BF16),
                pltpu.VMEM((nl - 1, lcap, cells, cells), BF16),
                pltpu.VMEM(((nd - 1) * cap + (nl - 1) * lcap, rows, cells), BF16),
                pltpu.VMEM(((nd - 1) * cap + (nl - 1) * lcap, rows, cells), BF16),
                pltpu.VMEM((2, 1, cells), F32),
                pltpu.VMEM((nd - 1, 1, cells), F32),
                pltpu.VMEM((last, 1, cells), F32),
                dma((2 if direct else 3,)),
            ],
            compiler_params=pltpu.CompilerParams(collective_id=0, has_side_effects=True),
        )(
            own_src,
            send_block[0, 0].T,
            send_target[0, 0].T,
            send_count[0],
            left_block[0, 0].T,
            left_target[0, 0].T,
            left_count[0],
            fields[0].transpose(1, 0, 2).reshape(comp * blocks, cells),
            own_weight[0],
            send_weight[0, 0],
            left_weight[0, 0],
        )
        remapped, totals = pl.pallas_call(
            finish,
            out_shape=(
                jax.ShapeDtypeStruct((comp * blocks, cells), F32),
                jax.ShapeDtypeStruct((comp,), F32),
            ),
            in_specs=[vmem, vmem],
            out_specs=(hbm, hbm),
        )(
            pltpu.with_memory_space_constraint(remapped, pltpu.VMEM),
            pltpu.with_memory_space_constraint(totals, pltpu.VMEM),
        )
        remapped = remapped.reshape(comp, blocks, cells).transpose(1, 0, 2)
        return remapped[None], totals

    in_specs = (
        P("level", "dev", None, None),
        P("level", "dev"),
        P("level", "dev", None, None),
        P("level", "dev", None, None),
        P("level", "dev", None, None),
        P("level", "dev", None),
        P("level", "dev", None, None, None, None),
        P("level", "dev", None, None),
        P("level", "dev", None, None),
        P("level", "dev", None),
        P("level", "dev", None, None, None, None),
    )
    out_specs = (P("level", "dev", None, None), P())
    return jax.shard_map(body, mesh=mesh, in_specs=in_specs, out_specs=out_specs, check_vma=False)
```
